8 devices in a mesh: dp: 2 (over z, y), sp: 4 (over x, core).
Axes of the slice: x: 2, y: 2, z: 1, core: 2. Of those that a mesh axis runs over, the one named last changes fastest.
Arguments:
- latents: bfloat16 [6, 96, 256, 768], P('dp', 'sp'), parts along dimension 0
- text_ctx: bfloat16 [6, 120, 768], P('dp'), parts along dimension 0
- modulation: float32 [6, 6, 768], P('dp'), parts along dimension 0
- pos_temporal: float32 [96, 768], replicated
- w_qkv_spatial: bfloat16 [3, 12, 64, 768], replicated
- w_out_spatial: bfloat16 [12, 64, 768], replicated
- w_qkv_temporal: bfloat16 [3, 12, 64, 768], replicated
- w_out_temporal: bfloat16 [12, 64, 768], replicated
- w_query_cross: bfloat16 [12, 64, 768], replicated
- w_kv_cross: bfloat16 [2, 12, 64, 768], replicated
- w_out_cross: bfloat16 [12, 64, 768], replicated
- w_mlp_in: bfloat16 [768, 3072], replicated
- w_mlp_out: bfloat16 [3072, 768], replicated
Outputs:
- output: bfloat16 [6, 96, 256, 768], P('dp', 'sp'), parts along dimension 0
There are 2 independent parts. The reference program is written for one: setup_inputs(seed, part) draws one part's arguments, and reference() takes and returns one part's arrays. A program takes and returns all parts, laid end to end along the dimension named above; an argument that names none is the same for every part.
All inputs are finite; a program needn't handle non-finite values.
Results may differ from the reference program's by a relative error of at most 0.0143476.
Values are sent between devices in bfloat16 or wider.
A program may use at most 1 GiB of HBM per device.

```python
import jax
import jax.numpy as jnp
from jax import lax

BATCH_SIZE = 3
NUM_FRAMES = 96
NUM_PATCHES = 256
MODEL_WIDTH = 768
NUM_HEADS = 12
TEXT_LEN = 120

HEAD_DIM = MODEL_WIDTH // NUM_HEADS
LN_EPS = 1e-6


def weight_draw(rng_key, arr_shape, fan_in):
    return (jax.random.normal(rng_key, arr_shape, jnp.float32) * (fan_in ** -0.5)).astype(jnp.bfloat16)


def setup_inputs(seed: int = 0, part: int = 0) -> dict:
    part_keys = jax.random.split(jax.random.fold_in(jax.random.key(seed), part), 6)
    shared_keys = jax.random.split(jax.random.key(seed + 1), 11)
    act_shape = (BATCH_SIZE, NUM_FRAMES, NUM_PATCHES, MODEL_WIDTH)
    token_base = jax.random.normal(part_keys[0], (BATCH_SIZE, 1, NUM_PATCHES, MODEL_WIDTH), jnp.float32)
    frame_base = jax.random.normal(part_keys[1], (BATCH_SIZE, NUM_FRAMES, 1, MODEL_WIDTH), jnp.float32)
    noise_part = jax.random.normal(part_keys[2], act_shape, jnp.float32)
    latents = (0.5 * token_base + 0.5 * frame_base + 0.6 * noise_part).astype(jnp.bfloat16)
    ctx_common = jax.random.normal(part_keys[3], (BATCH_SIZE, 1, MODEL_WIDTH), jnp.float32)
    ctx_noise = jax.random.normal(part_keys[4], (BATCH_SIZE, TEXT_LEN, MODEL_WIDTH), jnp.float32)
    text_ctx = (0.5 * ctx_common + ctx_noise).astype(jnp.bfloat16)
    gate_offset = jnp.array([0.0, 0.0, 1.0, 0.0, 0.0, 1.0], jnp.float32)[None, :, None]
    modulation = 0.3 * jax.random.normal(part_keys[5], (BATCH_SIZE, 6, MODEL_WIDTH), jnp.float32) + gate_offset
    pos_common = jax.random.normal(shared_keys[0], (1, MODEL_WIDTH), jnp.float32)
    pos_frames = jax.random.normal(shared_keys[1], (NUM_FRAMES, MODEL_WIDTH), jnp.float32)
    pos_temporal = 0.4 * pos_common + 0.4 * pos_frames
    head_shape = (NUM_HEADS, HEAD_DIM, MODEL_WIDTH)
    return {
        'latents': latents,
        'text_ctx': text_ctx,
        'modulation': modulation,
        'pos_temporal': pos_temporal,
        'w_qkv_spatial': weight_draw(shared_keys[2], (3,) + head_shape, MODEL_WIDTH),
        'w_out_spatial': weight_draw(shared_keys[3], head_shape, MODEL_WIDTH),
        'w_qkv_temporal': weight_draw(shared_keys[4], (3,) + head_shape, MODEL_WIDTH),
        'w_out_temporal': weight_draw(shared_keys[5], head_shape, MODEL_WIDTH),
        'w_query_cross': weight_draw(shared_keys[6], head_shape, MODEL_WIDTH),
        'w_kv_cross': weight_draw(shared_keys[7], (2,) + head_shape, MODEL_WIDTH),
        'w_out_cross': weight_draw(shared_keys[8], head_shape, MODEL_WIDTH),
        'w_mlp_in': weight_draw(shared_keys[9], (MODEL_WIDTH, 4 * MODEL_WIDTH), MODEL_WIDTH),
        'w_mlp_out': weight_draw(shared_keys[10], (4 * MODEL_WIDTH, MODEL_WIDTH), 4 * MODEL_WIDTH),
    }


def layer_norm(acts_in):
    centered = acts_in - jnp.mean(acts_in, axis=-1, keepdims=True)
    return centered * lax.rsqrt(jnp.mean(centered * centered, axis=-1, keepdims=True) + LN_EPS)


def attend(query_heads, key_heads, value_heads):
    scores = jnp.einsum('bqhd,bkhd->bhqk', query_heads.astype(jnp.float32), key_heads.astype(jnp.float32))
    attn_probs = jax.nn.softmax(scores * (HEAD_DIM ** -0.5), axis=-1).astype(jnp.bfloat16)
    mixed_out = jnp.einsum('bhqk,bkhd->bqhd', attn_probs.astype(jnp.float32), value_heads.astype(jnp.float32))
    return mixed_out.astype(jnp.bfloat16)


def qkv_proj(acts_in, weight):
    return jnp.einsum('bnc,jhdc->jbnhd', acts_in.astype(jnp.float32), weight.astype(jnp.float32)).astype(jnp.bfloat16)


def out_proj(mixed_in, weight):
    return jnp.einsum('bnhd,hdc->bnc', mixed_in.astype(jnp.float32), weight.astype(jnp.float32))


def reference(latents, text_ctx, modulation, pos_temporal, w_qkv_spatial, w_out_spatial, w_qkv_temporal, w_out_temporal, w_query_cross, w_kv_cross, w_out_cross, w_mlp_in, w_mlp_out):
    mod_rows = jnp.moveaxis(modulation, 1, 0)[:, :, None, :]

    def spatial_frame(frame_in):
        frame_f = frame_in.astype(jnp.float32)
        normed = (layer_norm(frame_f) * (1.0 + mod_rows[1]) + mod_rows[0]).astype(jnp.bfloat16)
        qkv_all = qkv_proj(normed, w_qkv_spatial)
        mixed_out = attend(qkv_all[0], qkv_all[1], qkv_all[2])
        return (frame_f + mod_rows[2] * out_proj(mixed_out, w_out_spatial)).astype(jnp.bfloat16)

    def temporal_patch(column_in):
        column_f = column_in.astype(jnp.float32)
        shifted = (column_f + pos_temporal[None]).astype(jnp.bfloat16)
        qkv_all = qkv_proj(shifted, w_qkv_temporal)
        mixed_out = attend(qkv_all[0], qkv_all[1], qkv_all[2])
        return (column_f + mod_rows[2] * out_proj(mixed_out, w_out_temporal)).astype(jnp.bfloat16)

    ctx_kv = qkv_proj(text_ctx, w_kv_cross)

    def cross_mlp_frame(frame_in):
        frame_f = frame_in.astype(jnp.float32)
        query_heads = qkv_proj(frame_in, w_query_cross[None])[0]
        mixed_out = attend(query_heads, ctx_kv[0], ctx_kv[1])
        after_cross = (frame_f + out_proj(mixed_out, w_out_cross)).astype(jnp.bfloat16)
        cross_f = after_cross.astype(jnp.float32)
        normed = (layer_norm(cross_f) * (1.0 + mod_rows[4]) + mod_rows[3]).astype(jnp.bfloat16)
        flat_rows = normed.reshape(-1, MODEL_WIDTH)
        mlp_hidden = jax.nn.gelu(jnp.dot(flat_rows, w_mlp_in, preferred_element_type=jnp.float32), approximate=True).astype(jnp.bfloat16)
        mlp_out = jnp.dot(mlp_hidden, w_mlp_out, preferred_element_type=jnp.float32).reshape(cross_f.shape)
        return (cross_f + mod_rows[5] * mlp_out).astype(jnp.bfloat16)

    after_spatial = lax.map(spatial_frame, jnp.moveaxis(latents, 1, 0))
    after_temporal = lax.map(temporal_patch, jnp.transpose(after_spatial, (2, 1, 0, 3)))
    out_frames = lax.map(cross_mlp_frame, jnp.transpose(after_temporal, (2, 1, 0, 3)))
    return jnp.moveaxis(out_frames, 0, 1)
```

```python
import functools
import math

import jax
import jax.numpy as jnp
from jax import lax
from jax.experimental import pallas as pl
from jax.experimental.pallas import tpu as pltpu
from jax.sharding import PartitionSpec as P

LN_EPS = 1e-6
F32 = jnp.float32
BF16 = jnp.bfloat16
LANES = 128
NEG = -1e30
GELU_C = math.sqrt(2.0 / math.pi)
SPATIAL_CHUNKS = (((0, 12), (12, 12)), ((0, 24),), ((0, 24),))
SPLITS = (2, 1, 1)
VMEM_LIMIT = 60 * 1024 * 1024

NT = (((1,), (1,)), ((), ()))
NN = (((1,), (0,)), ((), ()))


def dot(lhs, rhs, dims=NN):
    return lax.dot_general(lhs, rhs, dims, preferred_element_type=F32)


def normalize(rows):
    centered = rows - jnp.mean(rows, axis=-1, keepdims=True)
    return centered * lax.rsqrt(jnp.mean(centered * centered, axis=-1, keepdims=True) + LN_EPS)


def pair_masks(rows):
    lane = lax.broadcasted_iota(jnp.int32, (rows, LANES), 1)
    return lane < LANES // 2


def split_pair(block, low):
    zero = jnp.zeros_like(block)
    return jnp.where(low, block, zero), jnp.where(low, zero, block)


def spatial_kernel(head_dim, frames, steps, me_ref, x_ref, old_ref, mod_ref, wqkv_ref, wout_ref, *rest):
    outs, (u_ref, qkv_ref, s_ref, p_ref, inv_ref, att_ref, res_ref) = rest[:4], rest[4:]
    tokens, width = x_ref.shape[2], x_ref.shape[3]
    chunk = 2 * LANES
    chunks = width // chunk
    units = [(f, p) for f in range(frames) for p in range(2)]
    coef = math.log2(math.e) * head_dim ** -0.5
    low = pair_masks(tokens)

    def enter():
        for f in range(frames):
            u = normalize(x_ref[0, f].astype(F32)) * (1.0 + mod_ref[0, 1:2, :]) + mod_ref[0, 0:1, :]
            u_ref[f * tokens:(f + 1) * tokens, :] = u.astype(BF16)

    def project(j, c):
        cols = slice(j * width + c * chunk, j * width + (c + 1) * chunk)
        qkv_ref[:, cols] = dot(u_ref[...], wqkv_ref[:, cols]).astype(BF16)

    def block(j, c, f, p):
        c0 = j * width + c * chunk + p * LANES
        return qkv_ref[f * tokens:(f + 1) * tokens, c0:c0 + LANES]

    def scores(c):
        for n, (f, p) in enumerate(units):
            q = block(0, c, f, p)
            for h, kh in enumerate(split_pair(block(1, c, f, p), low)):
                s_ref[c % 2, n, h] = dot(q, kh, NT)

    def softmax(c):
        for n in range(len(units)):
            inv = []
            for h in range(2):
                s = s_ref[c % 2, n, h]
                e = jnp.exp2((s - jnp.max(s, axis=-1, keepdims=True)) * coef)
                inv.append(1.0 / jnp.sum(e, axis=-1, keepdims=True))
                p_ref[c % 2, n, :, h * tokens:(h + 1) * tokens] = e.astype(BF16)
            inv_ref[c % 2, n] = jnp.where(low, inv[0], inv[1])

    def values(c):
        for n, (f, p) in enumerate(units):
            o = dot(p_ref[c % 2, n], jnp.concatenate(split_pair(block(2, c, f, p), low), axis=0))
            c0 = c * chunk + p * LANES
            att_ref[f * tokens:(f + 1) * tokens, c0:c0 + LANES] = (o * inv_ref[c % 2, n]).astype(BF16)

    def leave():
        part = tokens // 4
        for c in range(chunks):
            cols = slice(c * chunk, (c + 1) * chunk)
            branch = mod_ref[0, 2:3, cols] * dot(att_ref[...], wout_ref[:, cols])
            for f in range(frames):
                rows = slice(f * tokens, (f + 1) * tokens)
                res_ref[rows, cols] = (old_ref[0, f, :, cols].astype(F32) + branch[rows]).astype(BF16)
        for f in range(frames):
            for r in range(4):
                start = pl.multiple_of((me_ref[0] ^ r) * part, part)
                outs[r][f] = res_ref[pl.ds(f * tokens + start, part), :]

    def step(first, last):
        if not last:
            enter()
        for c in range(chunks + 1):
            if c < chunks:
                if not first:
                    scores(c)
                if not last:
                    project(0, c)
                    project(1, c)
            if c > 0:
                if not first:
                    softmax(c - 1)
                    values(c - 1)
                if not last:
                    project(2, c - 1)
        if not first:
            leave()

    i = pl.program_id(0)
    pl.when(i == 0)(lambda: step(True, False))
    pl.when(jnp.logical_and(i > 0, i < steps))(lambda: step(False, False))
    pl.when(i == steps)(lambda: step(False, True))


def spatial_call(me, latents, modulation, wqkv, wout, video, first, count, head_dim, frames=2):
    tokens, width = latents.shape[2:]
    part = tokens // 4
    rows = frames * tokens
    steps = count // frames
    base = first // frames
    act = (1, frames, tokens, width)
    grid_spec = pltpu.PrefetchScalarGridSpec(
        num_scalar_prefetch=1,
        grid=(steps + 1,),
        in_specs=[
            pl.BlockSpec(act, lambda i, me: (video, base + jnp.minimum(i, steps - 1), 0, 0)),
            pl.BlockSpec(act, lambda i, me: (video, base + jnp.maximum(i - 1, 0), 0, 0)),
            pl.BlockSpec((1, 6, width), lambda i, me: (video, 0, 0)),
            pl.BlockSpec(wqkv.shape, lambda i, me: (0, 0)),
            pl.BlockSpec(wout.shape, lambda i, me: (0, 0)),
        ],
        out_specs=[pl.BlockSpec((frames, part, width), lambda i, me: (jnp.maximum(i - 1, 0), 0, 0))] * 4,
        scratch_shapes=[
            pltpu.VMEM((rows, width), BF16),
            pltpu.VMEM((rows, 3 * width), BF16),
            pltpu.VMEM((2, 2 * frames, 2, tokens, tokens), F32),
            pltpu.VMEM((2, 2 * frames, tokens, 2 * tokens), BF16),
            pltpu.VMEM((2, 2 * frames, tokens, LANES), F32),
            pltpu.VMEM((rows, width), BF16),
            pltpu.VMEM((rows, width), BF16),
        ],
    )
    total = count * tokens
    flops = 2 * total * (4 * width * width + 2 * tokens * width)
    return pl.pallas_call(
        functools.partial(spatial_kernel, head_dim, frames, steps),
        grid_spec=grid_spec,
        out_shape=[jax.ShapeDtypeStruct((count, part, width), BF16)] * 4,
        compiler_params=pltpu.CompilerParams(vmem_limit_bytes=VMEM_LIMIT),
        cost_estimate=pl.CostEstimate(flops=flops, bytes_accessed=4 * total * width, transcendentals=0),
        name=f"spatial_{video}_{first}",
    )(me, latents, latents, modulation, wqkv, wout)


def temporal_kernel(head_dim, pieces, patches, splits, me_ref, *refs):
    ins, refs = refs[:4 * pieces], refs[4 * pieces:]
    pos, refs = refs[:4 * pieces], refs[4 * pieces:]
    mod_ref, wqkv_ref, wout_ref = refs[:3]
    outs = refs[3:3 + 4 * splits]
    xf_ref, h_ref, qkv_ref, att_ref, s_ref, p_ref, inv_ref, pos_ref = refs[3 + 4 * splits:]
    per, _, width = ins[0].shape
    steps = 4 * pieces * per
    pairs = width // LANES
    pad = LANES - steps
    coef = math.log2(math.e) * head_dim ** -0.5
    blocks = [slice(c, c + LANES) for c in range(0, width, LANES)]
    lane_in, lane_out = patches + 1, steps + 1
    for n, ref in enumerate(ins):
        pos_ref[n * per:(n + 1) * per, :] = pos[n][0]
        for f in range(per):
            for c, cols in enumerate(blocks):
                xf_ref[c, (n * per + f) * lane_in:(n * per + f) * lane_in + patches, :] = ref[f, :, cols].astype(F32)
    group = 4
    for g in range(0, patches, group):
        for p in range(g, g + group):
            for c, cols in enumerate(blocks):
                h = xf_ref[c, pl.ds(p, steps, stride=lane_in), :]
                h_ref[p * steps:(p + 1) * steps, cols] = h.astype(BF16)
                att_ref[p * steps:(p + 1) * steps, cols] = (h + pos_ref[:, cols]).astype(BF16)
        rows = slice(g * steps, (g + group) * steps)
        qkv_ref[rows, :] = dot(att_ref[rows, :], wqkv_ref[...]).astype(BF16)
    low = pair_masks(steps)
    gap = jnp.zeros((pad, LANES), BF16)
    live = lax.broadcasted_iota(jnp.int32, (steps, LANES), 1) < steps

    def rows_of(p):
        return slice(p * steps, (p + 1) * steps)

    def scores(p, slot):
        rows = rows_of(p)
        for q in range(pairs):
            c0 = q * LANES
            k0, k1 = split_pair(qkv_ref[rows, width + c0:width + c0 + LANES], low)
            s_ref[slot, q] = dot(qkv_ref[rows, c0:c0 + LANES], jnp.concatenate([k0, gap, k1, gap], axis=0), NT)

    def softmax(slot):
        for q in range(pairs):
            inv = []
            for h in range(2):
                cols = slice(h * LANES, (h + 1) * LANES)
                sh = jnp.where(live, s_ref[slot, q, :, cols], NEG)
                e = jnp.exp2((sh - jnp.max(sh, axis=-1, keepdims=True)) * coef)
                inv.append(1.0 / jnp.sum(e, axis=-1, keepdims=True))
                p_ref[slot, q, :, cols] = e.astype(BF16)
            inv_ref[slot, q] = jnp.where(low, inv[0], inv[1])

    def values(p, slot):
        rows = rows_of(p)
        for q in range(pairs):
            c0 = q * LANES
            v0, v1 = split_pair(qkv_ref[rows, 2 * width + c0:2 * width + c0 + LANES], low)
            o = dot(p_ref[slot, q], jnp.concatenate([v0, gap, v1, gap], axis=0))
            att_ref[rows, c0:c0 + LANES] = (o * inv_ref[slot, q]).astype(BF16)

    scores(0, 0)
    scores(1, 1)
    softmax(0)

    for p in range(patches - 2):
        values(p, p % 2)
        softmax((p + 1) % 2)
        scores(p + 2, p % 2)
    values(patches - 2, 0)
    softmax(1)
    values(patches - 1, 1)
    wide = 2 * LANES
    for g in range(0, patches, group):
        rows = slice(g * steps, (g + group) * steps)
        for d in range(0, width, wide):
            branch = dot(att_ref[rows, :], wout_ref[:, d:d + wide])
            h2 = h_ref[rows, d:d + wide].astype(F32) + mod_ref[0, 2:3, d:d + wide] * branch
            for k in range(group):
                dst = slice((g + k) * lane_out, (g + k) * lane_out + steps)
                xf_ref[d // LANES, dst, :] = h2[k * steps:(k + 1) * steps, :LANES]
                xf_ref[d // LANES + 1, dst, :] = h2[k * steps:(k + 1) * steps, LANES:]
    span = pieces * per // splits
    for n in range(4 * pieces):
        for f in range(per):
            at = n // 4 * per + f
            ref = outs[at // span * 4 + n % 4]
            for c, cols in enumerate(blocks):
                ref[at % span, :, cols] = xf_ref[c, pl.ds(n * per + f, patches, stride=lane_out), :].astype(BF16)


def temporal_call(me, pieces, pos, modulation, wqkv, wout, video, splits, head_dim, patches=16):
    per, part, width = pieces[0].shape
    count = len(pieces) // 4
    steps = len(pieces) * per
    rows = steps * patches
    span = count * per // splits
    total = steps * part
    flops = 2 * total * (4 * width * width + 4 * LANES * width)
    pos = pos.reshape(4 * count, per, width)
    pos_spec = lambda r, h: pl.BlockSpec((1, per, width), lambda i, me: ((me[0] ^ r) * count + h, 0, 0))
    grid_spec = pltpu.PrefetchScalarGridSpec(
        num_scalar_prefetch=1,
        grid=(part // patches,),
        in_specs=[pl.BlockSpec((per, patches, width), lambda i, me: (0, i, 0))] * len(pieces)
        + [pos_spec(r, h) for h in range(count) for r in range(4)]
        + [
            pl.BlockSpec((1, 6, width), lambda i, me: (video, 0, 0)),
            pl.BlockSpec(wqkv.shape, lambda i, me: (0, 0)),
            pl.BlockSpec(wout.shape, lambda i, me: (0, 0)),
        ],
        out_specs=[pl.BlockSpec((span, patches, width), lambda i, me: (0, i, 0))] * (4 * splits),
        scratch_shapes=[
            pltpu.VMEM((width // LANES, rows + LANES, LANES), F32),
            pltpu.VMEM((rows, width), BF16),
            pltpu.VMEM((rows, 3 * width), BF16),
            pltpu.VMEM((rows, width), BF16),
            pltpu.VMEM((2, width // LANES, steps, 2 * LANES), F32),
            pltpu.VMEM((2, width // LANES, steps, 2 * LANES), BF16),
            pltpu.VMEM((2, width // LANES, steps, LANES), F32),
            pltpu.VMEM((steps, width), F32),
        ],
    )
    return pl.pallas_call(
        functools.partial(temporal_kernel, head_dim, count, patches, splits),
        grid_spec=grid_spec,
        out_shape=[jax.ShapeDtypeStruct((span, part, width), BF16)] * (4 * splits),
        compiler_params=pltpu.CompilerParams(vmem_limit_bytes=VMEM_LIMIT),
        cost_estimate=pl.CostEstimate(flops=flops, bytes_accessed=4 * total * width, transcendentals=0),
        name=f"temporal_{video}",
    )(me, *pieces, *([pos] * len(pieces)), modulation, wqkv, wout)


def cross_kernel(head_dim, frames, text_len, steps, me_ref, *refs):
    ins = refs[:4]
    mod_ref, kk_ref, vv_ref, wq_ref, wo_ref, win_ref, wmid_ref = refs[4:11]
    out_ref, h_ref, q_ref, s_ref, p_ref, inv_ref, att_ref, new_ref, h3_ref, n_ref, g_ref = refs[-11:]
    part, width = ins[0].shape[1:]
    tokens = 4 * part
    rows = frames * tokens
    hidden = win_ref.shape[1]
    pairs = width // LANES
    span = hidden // pairs
    wide = 2 * LANES
    coef = math.log2(math.e) * head_dim ** -0.5
    low = pair_masks(rows)
    live = lax.broadcasted_iota(jnp.int32, (rows, LANES), 1) < text_len

    def enter():
        for f in range(frames):
            for r in range(4):
                h_ref[f * tokens + r * part:f * tokens + (r + 1) * part, :] = ins[r][f]
        q_ref[...] = dot(h_ref[...], wq_ref[...]).astype(BF16)

    def scores(p):
        s_ref[p % 2] = dot(q_ref[:, p * LANES:(p + 1) * LANES], kk_ref[0, p], NT)

    def softmax(p):
        inv = []
        for h in range(2):
            cols = slice(h * LANES, (h + 1) * LANES)
            sh = jnp.where(live, s_ref[p % 2, :, cols], NEG)
            e = jnp.exp2((sh - jnp.max(sh, axis=-1, keepdims=True)) * coef)
            inv.append(1.0 / jnp.sum(e, axis=-1, keepdims=True))
            p_ref[p % 2, :, cols] = e.astype(BF16)
        inv_ref[p % 2] = jnp.where(low, inv[0], inv[1])

    def values(p):
        o = dot(p_ref[p % 2], vv_ref[0, p])
        att_ref[:, p * LANES:(p + 1) * LANES] = (o * inv_ref[p % 2]).astype(BF16)

    def expand(p):
        cols = slice(p * span, (p + 1) * span)
        a = dot(n_ref[...], win_ref[:, cols])
        t = jnp.tanh(a * (GELU_C + (GELU_C * 0.044715) * (a * a)))
        half = 0.5 * a
        g_ref[:, cols] = (half + half * t).astype(BF16)

    def attend_out():
        for d in range(0, width, wide):
            cols = slice(d, d + wide)
            new_ref[:, cols] = (h_ref[:, cols].astype(F32) + dot(att_ref[...], wo_ref[:, cols])).astype(BF16)

    def norm():
        n_ref[...] = (normalize(new_ref[...].astype(F32)) * (1.0 + mod_ref[0, 4:5, :]) + mod_ref[0, 3:4, :]).astype(BF16)

    def contract():
        for d in range(0, width, wide):
            cols = slice(d, d + wide)
            y = (h3_ref[:, cols].astype(F32) + mod_ref[0, 5:6, cols] * dot(g_ref[...], wmid_ref[:, cols])).astype(BF16)
            for f in range(frames):
                for r in range(4):
                    start = pl.multiple_of((me_ref[0] ^ r) * part, part)
                    out_ref[0, f, pl.ds(start, part), cols] = y[f * tokens + r * part:f * tokens + (r + 1) * part]

    def step(first, last):
        if not last:
            enter()
            scores(0)
        for p in range(pairs):
            if not last and p + 1 < pairs:
                scores(p + 1)
            if not first:
                expand(p)
            if not last:
                softmax(p)
                values(p)
        if not last:
            attend_out()
            norm()
        if not first:
            contract()
        if not last:
            h3_ref[...] = new_ref[...]

    i = pl.program_id(0)
    pl.when(i == 0)(lambda: step(True, False))
    pl.when(jnp.logical_and(i > 0, i < steps))(lambda: step(False, False))
    pl.when(i == steps)(lambda: step(False, True))


def cross_call(me, pieces, modulation, kk, vv, wq, wo, win, wmid, prev, out_shape, video, first, text_len, head_dim, frames=2):
    per, part, width = pieces[0].shape
    rows = frames * 4 * part
    hidden = win.shape[1]
    steps = per // frames
    base = first // frames
    whole = lambda a: pl.BlockSpec(a.shape, lambda i, me: (0, 0))
    in_specs = [pl.BlockSpec((frames, part, width), lambda i, me: (jnp.minimum(i, steps - 1), 0, 0))] * 4 + [
        pl.BlockSpec((1, 6, width), lambda i, me: (video, 0, 0)),
        pl.BlockSpec((1,) + kk.shape[1:], lambda i, me: (video, 0, 0, 0)),
        pl.BlockSpec((1,) + vv.shape[1:], lambda i, me: (video, 0, 0, 0)),
        whole(wq), whole(wo), whole(win), whole(wmid),
    ]
    args = [me, *pieces, modulation, kk, vv, wq, wo, win, wmid]
    aliases = {}
    if prev is not None:
        in_specs.append(pl.BlockSpec(memory_space=pl.ANY))
        aliases = {len(args): 0}
        args.append(prev)
    grid_spec = pltpu.PrefetchScalarGridSpec(
        num_scalar_prefetch=1,
        grid=(steps + 1,),
        in_specs=in_specs,
        out_specs=pl.BlockSpec((1, frames, 4 * part, width), lambda i, me: (video, base + jnp.maximum(i - 1, 0), 0, 0)),
        scratch_shapes=[
            pltpu.VMEM((rows, width), BF16),
            pltpu.VMEM((rows, width), BF16),
            pltpu.VMEM((2, rows, 2 * LANES), F32),
            pltpu.VMEM((2, rows, 2 * LANES), BF16),
            pltpu.VMEM((2, rows, LANES), F32),
            pltpu.VMEM((rows, width), BF16),
            pltpu.VMEM((rows, width), BF16),
            pltpu.VMEM((rows, width), BF16),
            pltpu.VMEM((rows, width), BF16),
            pltpu.VMEM((rows, hidden), BF16),
        ],
    )
    total = per * 4 * part
    flops = 2 * total * (2 * width * width + 4 * LANES * width + 2 * width * hidden)
    return pl.pallas_call(
        functools.partial(cross_kernel, head_dim, frames, text_len, steps),
        grid_spec=grid_spec,
        out_shape=jax.ShapeDtypeStruct(out_shape, BF16),
        input_output_aliases=aliases,
        compiler_params=pltpu.CompilerParams(vmem_limit_bytes=VMEM_LIMIT),
        cost_estimate=pl.CostEstimate(flops=flops, bytes_accessed=4 * total * width, transcendentals=0),
        name=f"cross_{video}_{first}",
    )(*args)


def text_kernel(ctx_ref, wkv_ref, kk_ref, vv_ref):
    length, width = ctx_ref.shape[1:]
    kv = dot(ctx_ref[0], wkv_ref[...], NT)
    kv = jnp.concatenate([kv, jnp.zeros((LANES - length, 2 * width), F32)], axis=0).astype(BF16)
    low = pair_masks(LANES)
    for p in range(width // LANES):
        for ref, c0 in ((kk_ref, p * LANES), (vv_ref, width + p * LANES)):
            for h, half in enumerate(split_pair(kv[:, c0:c0 + LANES], low)):
                ref[0, p, h * LANES:(h + 1) * LANES, :] = half


def text_blocks(text_ctx, w_kv):
    videos, length, width = text_ctx.shape
    block = (1, width // LANES, 2 * LANES, LANES)
    return pl.pallas_call(
        text_kernel,
        grid=(videos,),
        in_specs=[pl.BlockSpec((1, length, width), lambda b: (b, 0, 0)), pl.BlockSpec(w_kv.shape, lambda b: (0, 0))],
        out_specs=[pl.BlockSpec(block, lambda b: (b, 0, 0, 0))] * 2,
        out_shape=[jax.ShapeDtypeStruct((videos,) + block[1:], BF16)] * 2,
        compiler_params=pltpu.CompilerParams(vmem_limit_bytes=VMEM_LIMIT),
        cost_estimate=pl.CostEstimate(flops=4 * videos * LANES * width * width, bytes_accessed=w_kv.size * 2, transcendentals=0),
        name="text",
    )(text_ctx, w_kv)


def solution(mesh):
    act_spec = P('dp', 'sp', None, None)
    row_spec = P('dp', None, None)
    rep_two = P(None, None)
    rep_three = P(None, None, None)
    rep_four = P(None, None, None, None)
    in_specs = (act_spec, row_spec, row_spec, rep_two, rep_four, rep_three, rep_four, rep_three, rep_three, rep_four, rep_three, rep_two, rep_two)
    def exchange(parts):
        return [parts[0]] + [lax.ppermute(parts[r], 'sp', [(i, i ^ r) for i in range(4)]) for r in range(1, 4)]

    def local_block(latents, text_ctx, modulation, pos_temporal, w_qkv_spatial, w_out_spatial, w_qkv_temporal, w_out_temporal, w_query_cross, w_kv_cross, w_out_cross, w_mlp_in, w_mlp_out):
        videos, frames, tokens, width = latents.shape
        head_dim = w_out_spatial.shape[1]
        index = lax.axis_index('sp')
        me = index.astype(jnp.int32)[None]
        flat_in = lambda w: w.reshape(-1, width).T
        flat_out = lambda w: w.reshape(width, width)
        wqkv_s, wqkv_t, wq_c = flat_in(w_qkv_spatial), flat_in(w_qkv_temporal), flat_in(w_query_cross)
        wo_s, wo_t, wo_c = flat_out(w_out_spatial), flat_out(w_out_temporal), flat_out(w_out_cross)
        kk, vv = text_blocks(text_ctx, w_kv_cross.reshape(-1, width))
        gathered = []
        for b in range(videos):
            pieces = []
            for first, count in SPATIAL_CHUNKS[b]:
                pieces += exchange(spatial_call(me, latents, modulation, wqkv_s, wo_s, b, first, count, head_dim))
            gathered.append(pieces)
        returned = []
        for b in range(videos):
            splits = SPLITS[b]
            parts = temporal_call(me, gathered[b], pos_temporal, modulation, wqkv_t, wo_t, b, splits, head_dim)
            returned.append([exchange(parts[4 * n:4 * n + 4]) for n in range(splits)])
        y = None
        for b in range(videos):
            for n, pieces in enumerate(returned[b]):
                y = cross_call(me, pieces, modulation, kk, vv, wq_c, wo_c, w_mlp_in, w_mlp_out, y, latents.shape, b, n * frames // SPLITS[b], text_ctx.shape[1], head_dim)
        return y

    return jax.shard_map(local_block, mesh=mesh, in_specs=in_specs, out_specs=act_spec, check_vma=False)
```

```python
import functools
import math

import jax
import jax.numpy as jnp
from jax import lax
from jax.experimental import pallas as pl
from jax.experimental.pallas import tpu as pltpu
from jax.sharding import PartitionSpec as P

LN_EPS = 1e-6
F32 = jnp.float32
BF16 = jnp.bfloat16
LANES = 128
NEG = -1e30
GELU_C = math.sqrt(2.0 / math.pi)
SPATIAL_CHUNKS = (((0, 12), (12, 12)), ((0, 24),), ((0, 24),))
SPLITS = (2, 2, 1)
VMEM_LIMIT = 60 * 1024 * 1024

NT = (((1,), (1,)), ((), ()))
NN = (((1,), (0,)), ((), ()))


def dot(lhs, rhs, dims=NN):
    return lax.dot_general(lhs, rhs, dims, preferred_element_type=F32)


def normalize(rows):
    centered = rows - jnp.mean(rows, axis=-1, keepdims=True)
    return centered * lax.rsqrt(jnp.mean(centered * centered, axis=-1, keepdims=True) + LN_EPS)


def pair_masks(rows):
    lane = lax.broadcasted_iota(jnp.int32, (rows, LANES), 1)
    return lane < LANES // 2


def split_pair(block, low):
    zero = jnp.zeros_like(block)
    return jnp.where(low, block, zero), jnp.where(low, zero, block)


def spatial_kernel(head_dim, frames, steps, me_ref, x_ref, old_ref, mod_ref, wqkv_ref, wout_ref, *rest):
    outs, (u_ref, qkv_ref, s_ref, p_ref, inv_ref, att_ref, res_ref) = rest[:4], rest[4:]
    tokens, width = x_ref.shape[2], x_ref.shape[3]
    chunk = 2 * LANES
    chunks = width // chunk
    units = [(f, p) for f in range(frames) for p in range(2)]
    coef = math.log2(math.e) * head_dim ** -0.5
    low = pair_masks(tokens)

    def enter():
        for f in range(frames):
            u = normalize(x_ref[0, f].astype(F32)) * (1.0 + mod_ref[0, 1:2, :]) + mod_ref[0, 0:1, :]
            u_ref[f * tokens:(f + 1) * tokens, :] = u.astype(BF16)

    def project(j, c):
        cols = slice(j * width + c * chunk, j * width + (c + 1) * chunk)
        qkv_ref[:, cols] = dot(u_ref[...], wqkv_ref[cols, :], NT).astype(BF16)

    def block(j, c, f, p):
        c0 = j * width + c * chunk + p * LANES
        return qkv_ref[f * tokens:(f + 1) * tokens, c0:c0 + LANES]

    def scores(c):
        for n, (f, p) in enumerate(units):
            q = block(0, c, f, p)
            for h, kh in enumerate(split_pair(block(1, c, f, p), low)):
                s_ref[c % 2, n, h] = dot(q, kh, NT)

    def softmax(c):
        for n in range(len(units)):
            inv = []
            for h in range(2):
                s = s_ref[c % 2, n, h]
                e = jnp.exp2((s - jnp.max(s, axis=-1, keepdims=True)) * coef)
                inv.append(1.0 / jnp.sum(e, axis=-1, keepdims=True))
                p_ref[c % 2, n, :, h * tokens:(h + 1) * tokens] = e.astype(BF16)
            inv_ref[c % 2, n] = jnp.where(low, inv[0], inv[1])

    def values(c):
        for n, (f, p) in enumerate(units):
            o = dot(p_ref[c % 2, n], jnp.concatenate(split_pair(block(2, c, f, p), low), axis=0))
            c0 = c * chunk + p * LANES
            att_ref[f * tokens:(f + 1) * tokens, c0:c0 + LANES] = (o * inv_ref[c % 2, n]).astype(BF16)

    def leave():
        part = tokens // 4
        for c in range(chunks):
            cols = slice(c * chunk, (c + 1) * chunk)
            branch = mod_ref[0, 2:3, cols] * dot(att_ref[...], wout_ref[:, cols])
            for f in range(frames):
                rows = slice(f * tokens, (f + 1) * tokens)
                res_ref[rows, cols] = (old_ref[0, f, :, cols].astype(F32) + branch[rows]).astype(BF16)
        for f in range(frames):
            for r in range(4):
                start = pl.multiple_of((me_ref[0] ^ r) * part, part)
                outs[r][f] = res_ref[pl.ds(f * tokens + start, part), :]

    def step(first, last):
        if not last:
            enter()
        for c in range(chunks + 1):
            if c < chunks:
                if not first:
                    scores(c)
                if not last:
                    project(0, c)
                    project(1, c)
            if c > 0:
                if not first:
                    softmax(c - 1)
                    values(c - 1)
                if not last:
                    project(2, c - 1)
        if not first:
            leave()

    i = pl.program_id(0)
    pl.when(i == 0)(lambda: step(True, False))
    pl.when(jnp.logical_and(i > 0, i < steps))(lambda: step(False, False))
    pl.when(i == steps)(lambda: step(False, True))


def spatial_call(me, latents, modulation, wqkv, wout, video, first, count, head_dim, frames=2):
    tokens, width = latents.shape[2:]
    part = tokens // 4
    rows = frames * tokens
    steps = count // frames
    base = first // frames
    act = (1, frames, tokens, width)
    grid_spec = pltpu.PrefetchScalarGridSpec(
        num_scalar_prefetch=1,
        grid=(steps + 1,),
        in_specs=[
            pl.BlockSpec(act, lambda i, me: (video, base + jnp.minimum(i, steps - 1), 0, 0)),
            pl.BlockSpec(act, lambda i, me: (video, base + jnp.maximum(i - 1, 0), 0, 0)),
            pl.BlockSpec((1, 6, width), lambda i, me: (video, 0, 0)),
            pl.BlockSpec(wqkv.shape, lambda i, me: (0, 0)),
            pl.BlockSpec(wout.shape, lambda i, me: (0, 0)),
        ],
        out_specs=[pl.BlockSpec((frames, part, width), lambda i, me: (jnp.maximum(i - 1, 0), 0, 0))] * 4,
        scratch_shapes=[
            pltpu.VMEM((rows, width), BF16),
            pltpu.VMEM((rows, 3 * width), BF16),
            pltpu.VMEM((2, 2 * frames, 2, tokens, tokens), F32),
            pltpu.VMEM((2, 2 * frames, tokens, 2 * tokens), BF16),
            pltpu.VMEM((2, 2 * frames, tokens, LANES), F32),
            pltpu.VMEM((rows, width), BF16),
            pltpu.VMEM((rows, width), BF16),
        ],
    )
    total = count * tokens
    flops = 2 * total * (4 * width * width + 2 * tokens * width)
    return pl.pallas_call(
        functools.partial(spatial_kernel, head_dim, frames, steps),
        grid_spec=grid_spec,
        out_shape=[jax.ShapeDtypeStruct((count, part, width), BF16)] * 4,
        compiler_params=pltpu.CompilerParams(vmem_limit_bytes=VMEM_LIMIT),
        cost_estimate=pl.CostEstimate(flops=flops, bytes_accessed=4 * total * width, transcendentals=0),
        name=f"spatial_{video}_{first}",
    )(me, latents, latents, modulation, wqkv, wout)


def temporal_kernel(head_dim, pieces, patches, splits, me_ref, *refs):
    ins, refs = refs[:4 * pieces], refs[4 * pieces:]
    pos, refs = refs[:4], refs[4:]
    mod_ref, wqkv_ref, wout_ref = refs[:3]
    outs = refs[3:3 + 4 * splits]
    xf_ref, h_ref, qkv_ref, att_ref, s_ref, p_ref, inv_ref, pos_ref = refs[3 + 4 * splits:]
    per, _, width = ins[0].shape
    steps = 4 * pieces * per
    pairs = width // LANES
    pad = LANES - steps
    coef = math.log2(math.e) * head_dim ** -0.5
    blocks = [slice(c, c + LANES) for c in range(0, width, LANES)]
    lane_in, lane_out = patches + 1, steps + 1
    for n, ref in enumerate(ins):
        pos_ref[n * per:(n + 1) * per, :] = pos[n % 4][n // 4 * per:(n // 4 + 1) * per, :]
        for f in range(per):
            for c, cols in enumerate(blocks):
                xf_ref[c, (n * per + f) * lane_in:(n * per + f) * lane_in + patches, :] = ref[f, :, cols].astype(F32)
    group = 4
    for g in range(0, patches, group):
        for p in range(g, g + group):
            for c, cols in enumerate(blocks):
                h = xf_ref[c, pl.ds(p, steps, stride=lane_in), :]
                h_ref[p * steps:(p + 1) * steps, cols] = h.astype(BF16)
                att_ref[p * steps:(p + 1) * steps, cols] = (h + pos_ref[:, cols]).astype(BF16)
        rows = slice(g * steps, (g + group) * steps)
        qkv_ref[rows, :] = dot(att_ref[rows, :], wqkv_ref[...], NT).astype(BF16)
    low = pair_masks(steps)
    gap = jnp.zeros((pad, LANES), BF16)
    live = lax.broadcasted_iota(jnp.int32, (steps, LANES), 1) < steps

    def rows_of(p):
        return slice(p * steps, (p + 1) * steps)

    def scores(p, slot):
        rows = rows_of(p)
        for q in range(pairs):
            c0 = q * LANES
            k0, k1 = split_pair(qkv_ref[rows, width + c0:width + c0 + LANES], low)
            s_ref[slot, q] = dot(qkv_ref[rows, c0:c0 + LANES], jnp.concatenate([k0, gap, k1, gap], axis=0), NT)

    def softmax(slot):
        for q in range(pairs):
            inv = []
            for h in range(2):
                cols = slice(h * LANES, (h + 1) * LANES)
                sh = jnp.where(live, s_ref[slot, q, :, cols], NEG)
                e = jnp.exp2((sh - jnp.max(sh, axis=-1, keepdims=True)) * coef)
                inv.append(1.0 / jnp.sum(e, axis=-1, keepdims=True))
                p_ref[slot, q, :, cols] = e.astype(BF16)
            inv_ref[slot, q] = jnp.where(low, inv[0], inv[1])

    def values(p, slot):
        rows = rows_of(p)
        for q in range(pairs):
            c0 = q * LANES
            v0, v1 = split_pair(qkv_ref[rows, 2 * width + c0:2 * width + c0 + LANES], low)
            o = dot(p_ref[slot, q], jnp.concatenate([v0, gap, v1, gap], axis=0))
            att_ref[rows, c0:c0 + LANES] = (o * inv_ref[slot, q]).astype(BF16)

    scores(0, 0)
    scores(1, 1)
    softmax(0)

    for p in range(patches - 2):
        values(p, p % 2)
        softmax((p + 1) % 2)
        scores(p + 2, p % 2)
    values(patches - 2, 0)
    softmax(1)
    values(patches - 1, 1)
    wide = 2 * LANES
    for g in range(0, patches, group):
        rows = slice(g * steps, (g + group) * steps)
        for d in range(0, width, wide):
            branch = dot(att_ref[rows, :], wout_ref[:, d:d + wide])
            h2 = h_ref[rows, d:d + wide].astype(F32) + mod_ref[0, 2:3, d:d + wide] * branch
            for k in range(group):
                dst = slice((g + k) * lane_out, (g + k) * lane_out + steps)
                xf_ref[d // LANES, dst, :] = h2[k * steps:(k + 1) * steps, :LANES]
                xf_ref[d // LANES + 1, dst, :] = h2[k * steps:(k + 1) * steps, LANES:]
    span = pieces * per // splits
    for n in range(4 * pieces):
        for f in range(per):
            at = n // 4 * per + f
            ref = outs[at // span * 4 + n % 4]
            for c, cols in enumerate(blocks):
                ref[at % span, :, cols] = xf_ref[c, pl.ds(n * per + f, patches, stride=lane_out), :].astype(BF16)


def temporal_call(me, pieces, pos, modulation, wqkv, wout, video, splits, head_dim, patches=16):
    per, part, width = pieces[0].shape
    count = len(pieces) // 4
    steps = len(pieces) * per
    rows = steps * patches
    span = count * per // splits
    total = steps * part
    flops = 2 * total * (4 * width * width + 4 * LANES * width)
    pos_spec = lambda r: pl.BlockSpec((count * per, width), lambda i, me: (me[0] ^ r, 0))
    grid_spec = pltpu.PrefetchScalarGridSpec(
        num_scalar_prefetch=1,
        grid=(part // patches,),
        in_specs=[pl.BlockSpec((per, patches, width), lambda i, me: (0, i, 0))] * len(pieces)
        + [pos_spec(r) for r in range(4)]
        + [
            pl.BlockSpec((1, 6, width), lambda i, me: (video, 0, 0)),
            pl.BlockSpec(wqkv.shape, lambda i, me: (0, 0)),
            pl.BlockSpec(wout.shape, lambda i, me: (0, 0)),
        ],
        out_specs=[pl.BlockSpec((span, patches, width), lambda i, me: (0, i, 0))] * (4 * splits),
        scratch_shapes=[
            pltpu.VMEM((width // LANES, rows + LANES, LANES), F32),
            pltpu.VMEM((rows, width), BF16),
            pltpu.VMEM((rows, 3 * width), BF16),
            pltpu.VMEM((rows, width), BF16),
            pltpu.VMEM((2, width // LANES, steps, 2 * LANES), F32),
            pltpu.VMEM((2, width // LANES, steps, 2 * LANES), BF16),
            pltpu.VMEM((2, width // LANES, steps, LANES), F32),
            pltpu.VMEM((steps, width), F32),
        ],
    )
    return pl.pallas_call(
        functools.partial(temporal_kernel, head_dim, count, patches, splits),
        grid_spec=grid_spec,
        out_shape=[jax.ShapeDtypeStruct((span, part, width), BF16)] * (4 * splits),
        compiler_params=pltpu.CompilerParams(vmem_limit_bytes=VMEM_LIMIT),
        cost_estimate=pl.CostEstimate(flops=flops, bytes_accessed=4 * total * width, transcendentals=0),
        name=f"temporal_{video}",
    )(me, *pieces, *([pos] * 4), modulation, wqkv, wout)


def cross_kernel(head_dim, frames, text_len, steps, me_ref, *refs):
    ins = refs[:4]
    mod_ref, kk_ref, vv_ref, wq_ref, wo_ref, win_ref, wmid_ref = refs[4:11]
    out_ref, h_ref, q_ref, s_ref, p_ref, inv_ref, att_ref, new_ref, h3_ref, n_ref, g_ref = refs[-11:]
    part, width = ins[0].shape[1:]
    tokens = 4 * part
    rows = frames * tokens
    hidden = win_ref.shape[1]
    pairs = width // LANES
    span = hidden // pairs
    wide = 2 * LANES
    coef = math.log2(math.e) * head_dim ** -0.5
    low = pair_masks(rows)
    live = lax.broadcasted_iota(jnp.int32, (rows, LANES), 1) < text_len

    def enter():
        for f in range(frames):
            for r in range(4):
                h_ref[f * tokens + r * part:f * tokens + (r + 1) * part, :] = ins[r][f]
        q_ref[...] = dot(h_ref[...], wq_ref[...], NT).astype(BF16)

    def scores(p):
        s_ref[p % 2] = dot(q_ref[:, p * LANES:(p + 1) * LANES], kk_ref[0, p], NT)

    def softmax(p):
        inv = []
        for h in range(2):
            cols = slice(h * LANES, (h + 1) * LANES)
            sh = jnp.where(live, s_ref[p % 2, :, cols], NEG)
            e = jnp.exp2((sh - jnp.max(sh, axis=-1, keepdims=True)) * coef)
            inv.append(1.0 / jnp.sum(e, axis=-1, keepdims=True))
            p_ref[p % 2, :, cols] = e.astype(BF16)
        inv_ref[p % 2] = jnp.where(low, inv[0], inv[1])

    def values(p):
        o = dot(p_ref[p % 2], vv_ref[0, p])
        att_ref[:, p * LANES:(p + 1) * LANES] = (o * inv_ref[p % 2]).astype(BF16)

    def expand(p):
        cols = slice(p * span, (p + 1) * span)
        a = dot(n_ref[...], win_ref[:, cols])
        t = jnp.tanh(a * (GELU_C + (GELU_C * 0.044715) * (a * a)))
        half = 0.5 * a
        g_ref[:, cols] = (half + half * t).astype(BF16)

    def attend_out():
        for d in range(0, width, wide):
            cols = slice(d, d + wide)
            new_ref[:, cols] = (h_ref[:, cols].astype(F32) + dot(att_ref[...], wo_ref[:, cols])).astype(BF16)

    def norm():
        n_ref[...] = (normalize(new_ref[...].astype(F32)) * (1.0 + mod_ref[0, 4:5, :]) + mod_ref[0, 3:4, :]).astype(BF16)

    def contract():
        for d in range(0, width, wide):
            cols = slice(d, d + wide)
            y = (h3_ref[:, cols].astype(F32) + mod_ref[0, 5:6, cols] * dot(g_ref[...], wmid_ref[:, cols])).astype(BF16)
            for f in range(frames):
                for r in range(4):
                    start = pl.multiple_of((me_ref[0] ^ r) * part, part)
                    out_ref[0, f, pl.ds(start, part), cols] = y[f * tokens + r * part:f * tokens + (r + 1) * part]

    def step(first, last):
        if not last:
            enter()
            scores(0)
        for p in range(pairs):
            if not last and p + 1 < pairs:
                scores(p + 1)
            if not first:
                expand(p)
            if not last:
                softmax(p)
                values(p)
        if not last:
            attend_out()
            norm()
        if not first:
            contract()
        if not last:
            h3_ref[...] = new_ref[...]

    i = pl.program_id(0)
    pl.when(i == 0)(lambda: step(True, False))
    pl.when(jnp.logical_and(i > 0, i < steps))(lambda: step(False, False))
    pl.when(i == steps)(lambda: step(False, True))


def cross_call(me, pieces, modulation, kk, vv, wq, wo, win, wmid, prev, out_shape, video, first, text_len, head_dim, frames=2):
    per, part, width = pieces[0].shape
    rows = frames * 4 * part
    hidden = win.shape[1]
    steps = per // frames
    base = first // frames
    whole = lambda a: pl.BlockSpec(a.shape, lambda i, me: (0, 0))
    in_specs = [pl.BlockSpec((frames, part, width), lambda i, me: (jnp.minimum(i, steps - 1), 0, 0))] * 4 + [
        pl.BlockSpec((1, 6, width), lambda i, me: (video, 0, 0)),
        pl.BlockSpec((1,) + kk.shape[1:], lambda i, me: (video, 0, 0, 0)),
        pl.BlockSpec((1,) + vv.shape[1:], lambda i, me: (video, 0, 0, 0)),
        whole(wq), whole(wo), whole(win), whole(wmid),
    ]
    args = [me, *pieces, modulation, kk, vv, wq, wo, win, wmid]
    aliases = {}
    if prev is not None:
        in_specs.append(pl.BlockSpec(memory_space=pl.ANY))
        aliases = {len(args): 0}
        args.append(prev)
    grid_spec = pltpu.PrefetchScalarGridSpec(
        num_scalar_prefetch=1,
        grid=(steps + 1,),
        in_specs=in_specs,
        out_specs=pl.BlockSpec((1, frames, 4 * part, width), lambda i, me: (video, base + jnp.maximum(i - 1, 0), 0, 0)),
        scratch_shapes=[
            pltpu.VMEM((rows, width), BF16),
            pltpu.VMEM((rows, width), BF16),
            pltpu.VMEM((2, rows, 2 * LANES), F32),
            pltpu.VMEM((2, rows, 2 * LANES), BF16),
            pltpu.VMEM((2, rows, LANES), F32),
            pltpu.VMEM((rows, width), BF16),
            pltpu.VMEM((rows, width), BF16),
            pltpu.VMEM((rows, width), BF16),
            pltpu.VMEM((rows, width), BF16),
            pltpu.VMEM((rows, hidden), BF16),
        ],
    )
    total = per * 4 * part
    flops = 2 * total * (2 * width * width + 4 * LANES * width + 2 * width * hidden)
    return pl.pallas_call(
        functools.partial(cross_kernel, head_dim, frames, text_len, steps),
        grid_spec=grid_spec,
        out_shape=jax.ShapeDtypeStruct(out_shape, BF16),
        input_output_aliases=aliases,
        compiler_params=pltpu.CompilerParams(vmem_limit_bytes=VMEM_LIMIT),
        cost_estimate=pl.CostEstimate(flops=flops, bytes_accessed=4 * total * width, transcendentals=0),
        name=f"cross_{video}_{first}",
    )(*args)


def text_kernel(ctx_ref, wkv_ref, kk_ref, vv_ref):
    length, width = ctx_ref.shape[1:]
    kv = dot(ctx_ref[0], wkv_ref[...], NT)
    kv = jnp.concatenate([kv, jnp.zeros((LANES - length, 2 * width), F32)], axis=0).astype(BF16)
    low = pair_masks(LANES)
    for p in range(width // LANES):
        for ref, c0 in ((kk_ref, p * LANES), (vv_ref, width + p * LANES)):
            for h, half in enumerate(split_pair(kv[:, c0:c0 + LANES], low)):
                ref[0, p, h * LANES:(h + 1) * LANES, :] = half


def text_blocks(text_ctx, w_kv):
    videos, length, width = text_ctx.shape
    block = (1, width // LANES, 2 * LANES, LANES)
    return pl.pallas_call(
        text_kernel,
        grid=(videos,),
        in_specs=[pl.BlockSpec((1, length, width), lambda b: (b, 0, 0)), pl.BlockSpec(w_kv.shape, lambda b: (0, 0))],
        out_specs=[pl.BlockSpec(block, lambda b: (b, 0, 0, 0))] * 2,
        out_shape=[jax.ShapeDtypeStruct((videos,) + block[1:], BF16)] * 2,
        compiler_params=pltpu.CompilerParams(vmem_limit_bytes=VMEM_LIMIT),
        cost_estimate=pl.CostEstimate(flops=4 * videos * LANES * width * width, bytes_accessed=w_kv.size * 2, transcendentals=0),
        name="text",
    )(text_ctx, w_kv)


def solution(mesh):
    act_spec = P('dp', 'sp', None, None)
    row_spec = P('dp', None, None)
    rep_two = P(None, None)
    rep_three = P(None, None, None)
    rep_four = P(None, None, None, None)
    in_specs = (act_spec, row_spec, row_spec, rep_two, rep_four, rep_three, rep_four, rep_three, rep_three, rep_four, rep_three, rep_two, rep_two)
    def exchange(parts):
        return [parts[0]] + [lax.ppermute(parts[r], 'sp', [(i, i ^ r) for i in range(4)]) for r in range(1, 4)]

    def local_block(latents, text_ctx, modulation, pos_temporal, w_qkv_spatial, w_out_spatial, w_qkv_temporal, w_out_temporal, w_query_cross, w_kv_cross, w_out_cross, w_mlp_in, w_mlp_out):
        videos, frames, tokens, width = latents.shape
        head_dim = w_out_spatial.shape[1]
        index = lax.axis_index('sp')
        me = index.astype(jnp.int32)[None]
        flat_in = lambda w: w.reshape(-1, width)
        flat_out = lambda w: w.reshape(width, width)
        wqkv_s, wqkv_t, wq_c = flat_in(w_qkv_spatial), flat_in(w_qkv_temporal), flat_in(w_query_cross)
        wo_s, wo_t, wo_c = flat_out(w_out_spatial), flat_out(w_out_temporal), flat_out(w_out_cross)
        kk, vv = text_blocks(text_ctx, w_kv_cross.reshape(-1, width))
        gathered = []
        for b in range(videos):
            pieces = []
            for first, count in SPATIAL_CHUNKS[b]:
                parts = spatial_call(me, latents, modulation, wqkv_s, wo_s, b, first, count, head_dim)
                me, parts = lax.optimization_barrier((me, parts))
                pieces += exchange(parts)
            gathered.append(pieces)
        waiting, returned = [], {}

        def send_next(me):
            if waiting:
                key, parts = waiting.pop(0)
                me, parts = lax.optimization_barrier((me, parts))
                returned[key] = exchange(parts)
            return me

        for b in range(videos):
            parts = temporal_call(me, gathered[b], pos_temporal, modulation, wqkv_t, wo_t, b, SPLITS[b], head_dim)
            me, parts = lax.optimization_barrier((me, parts))
            waiting += [((b, n), parts[4 * n:4 * n + 4]) for n in range(SPLITS[b])]
            me = send_next(me)
        y = None
        for b in range(videos):
            for n in range(SPLITS[b]):
                y = cross_call(me, returned[b, n], modulation, kk, vv, wq_c, wo_c, w_mlp_in, w_mlp_out, y, latents.shape, b, n * frames // SPLITS[b], text_ctx.shape[1], head_dim)
                if waiting:
                    me, y = lax.optimization_barrier((me, y))
                    me = send_next(me)
        return y

    return jax.shard_map(local_block, mesh=mesh, in_specs=in_specs, out_specs=act_spec, check_vma=False)
```

```python
import functools
import math

import jax
import jax.numpy as jnp
from jax import lax
from jax.experimental import pallas as pl
from jax.experimental.pallas import tpu as pltpu
from jax.sharding import PartitionSpec as P

LN_EPS = 1e-6
F32 = jnp.float32
BF16 = jnp.bfloat16
LANES = 128
NEG = -1e30
GELU_C = math.sqrt(2.0 / math.pi)
SPATIAL_CHUNKS = (((0, 12), (12, 12)), ((0, 24),), ((0, 24),))
SPLITS = (2, 2, 1)
VMEM_LIMIT = 60 * 1024 * 1024

NT = (((1,), (1,)), ((), ()))
NN = (((1,), (0,)), ((), ()))


def dot(lhs, rhs, dims=NN):
    return lax.dot_general(lhs, rhs, dims, preferred_element_type=F32)


def normalize(rows):
    centered = rows - jnp.mean(rows, axis=-1, keepdims=True)
    return centered * lax.rsqrt(jnp.mean(centered * centered, axis=-1, keepdims=True) + LN_EPS)


def pair_masks(rows):
    lane = lax.broadcasted_iota(jnp.int32, (rows, LANES), 1)
    return lane < LANES // 2


def split_pair(block, low):
    zero = jnp.zeros_like(block)
    return jnp.where(low, block, zero), jnp.where(low, zero, block)


def spatial_kernel(head_dim, frames, steps, me_ref, x_ref, old_ref, mod_ref, wqkv_ref, wout_ref, *rest):
    outs, (u_ref, qkv_ref, s_ref, p_ref, inv_ref, att_ref, res_ref) = rest[:4], rest[4:]
    tokens, width = x_ref.shape[2], x_ref.shape[3]
    chunk = 2 * LANES
    chunks = width // chunk
    units = [(f, p) for f in range(frames) for p in range(2)]
    coef = math.log2(math.e) * head_dim ** -0.5
    low = pair_masks(tokens)

    def enter():
        for f in range(frames):
            u = normalize(x_ref[0, f].astype(F32)) * (1.0 + mod_ref[0, 1:2, :]) + mod_ref[0, 0:1, :]
            u_ref[f * tokens:(f + 1) * tokens, :] = u.astype(BF16)

    def project(j, c):
        cols = slice(j * width + c * chunk, j * width + (c + 1) * chunk)
        qkv_ref[:, cols] = dot(u_ref[...], wqkv_ref[cols, :], NT).astype(BF16)

    def block(j, c, f, p):
        c0 = j * width + c * chunk + p * LANES
        return qkv_ref[f * tokens:(f + 1) * tokens, c0:c0 + LANES]

    def scores(c):
        for n, (f, p) in enumerate(units):
            q = block(0, c, f, p)
            for h, kh in enumerate(split_pair(block(1, c, f, p), low)):
                s_ref[c % 2, n, h] = dot(q, kh, NT)

    def softmax(c):
        for n in range(len(units)):
            inv = []
            for h in range(2):
                s = s_ref[c % 2, n, h]
                e = jnp.exp2((s - jnp.max(s, axis=-1, keepdims=True)) * coef)
                inv.append(1.0 / jnp.sum(e, axis=-1, keepdims=True))
                p_ref[c % 2, n, :, h * tokens:(h + 1) * tokens] = e.astype(BF16)
            inv_ref[c % 2, n] = jnp.where(low, inv[0], inv[1])

    def values(c):
        for n, (f, p) in enumerate(units):
            o = dot(p_ref[c % 2, n], jnp.concatenate(split_pair(block(2, c, f, p), low), axis=0))
            c0 = c * chunk + p * LANES
            att_ref[f * tokens:(f + 1) * tokens, c0:c0 + LANES] = (o * inv_ref[c % 2, n]).astype(BF16)

    def leave():
        part = tokens // 4
        for c in range(chunks):
            cols = slice(c * chunk, (c + 1) * chunk)
            branch = mod_ref[0, 2:3, cols] * dot(att_ref[...], wout_ref[:, cols])
            for f in range(frames):
                rows = slice(f * tokens, (f + 1) * tokens)
                res_ref[rows, cols] = (old_ref[0, f, :, cols].astype(F32) + branch[rows]).astype(BF16)
        for f in range(frames):
            for r in range(4):
                start = pl.multiple_of((me_ref[0] ^ r) * part, part)
                outs[r][f] = res_ref[pl.ds(f * tokens + start, part), :]

    def step(first, last):
        if not last:
            enter()
        for c in range(chunks + 1):
            if c < chunks:
                if not first:
                    scores(c)
                if not last:
                    project(0, c)
                    project(1, c)
            if c > 0:
                if not first:
                    softmax(c - 1)
                    values(c - 1)
                if not last:
                    project(2, c - 1)
        if not first:
            leave()

    i = pl.program_id(0)
    pl.when(i == 0)(lambda: step(True, False))
    pl.when(jnp.logical_and(i > 0, i < steps))(lambda: step(False, False))
    pl.when(i == steps)(lambda: step(False, True))


def spatial_call(me, latents, modulation, wqkv, wout, video, first, count, head_dim, frames=2):
    tokens, width = latents.shape[2:]
    part = tokens // 4
    rows = frames * tokens
    steps = count // frames
    base = first // frames
    act = (1, frames, tokens, width)
    grid_spec = pltpu.PrefetchScalarGridSpec(
        num_scalar_prefetch=1,
        grid=(steps + 1,),
        in_specs=[
            pl.BlockSpec(act, lambda i, me: (video, base + jnp.minimum(i, steps - 1), 0, 0)),
            pl.BlockSpec(act, lambda i, me: (video, base + jnp.maximum(i - 1, 0), 0, 0)),
            pl.BlockSpec((1, 6, width), lambda i, me: (video, 0, 0)),
            pl.BlockSpec(wqkv.shape, lambda i, me: (0, 0)),
            pl.BlockSpec(wout.shape, lambda i, me: (0, 0)),
        ],
        out_specs=[pl.BlockSpec((frames, part, width), lambda i, me: (jnp.maximum(i - 1, 0), 0, 0))] * 4,
        scratch_shapes=[
            pltpu.VMEM((rows, width), BF16),
            pltpu.VMEM((rows, 3 * width), BF16),
            pltpu.VMEM((2, 2 * frames, 2, tokens, tokens), F32),
            pltpu.VMEM((2, 2 * frames, tokens, 2 * tokens), BF16),
            pltpu.VMEM((2, 2 * frames, tokens, LANES), F32),
            pltpu.VMEM((rows, width), BF16),
            pltpu.VMEM((rows, width), BF16),
        ],
    )
    total = count * tokens
    flops = 2 * total * (4 * width * width + 2 * tokens * width)
    return pl.pallas_call(
        functools.partial(spatial_kernel, head_dim, frames, steps),
        grid_spec=grid_spec,
        out_shape=[jax.ShapeDtypeStruct((count, part, width), BF16)] * 4,
        compiler_params=pltpu.CompilerParams(vmem_limit_bytes=VMEM_LIMIT),
        cost_estimate=pl.CostEstimate(flops=flops, bytes_accessed=4 * total * width, transcendentals=0),
        name=f"spatial_{video}_{first}",
    )(me, latents, latents, modulation, wqkv, wout)


def temporal_kernel(head_dim, pieces, patches, splits, me_ref, *refs):
    ins, refs = refs[:4 * pieces], refs[4 * pieces:]
    pos, refs = refs[:4], refs[4:]
    mod_ref, wqkv_ref, wout_ref = refs[:3]
    outs = refs[3:3 + 4 * splits]
    xf_ref, h_ref, qkv_ref, att_ref, s_ref, p_ref, inv_ref, pos_ref = refs[3 + 4 * splits:]
    per, _, width = ins[0].shape
    steps = 4 * pieces * per
    pairs = width // LANES
    pad = LANES - steps
    coef = math.log2(math.e) * head_dim ** -0.5
    blocks = [slice(c, c + LANES) for c in range(0, width, LANES)]
    lane_in, lane_out = patches + 1, steps + 1
    for n, ref in enumerate(ins):
        pos_ref[n * per:(n + 1) * per, :] = pos[n % 4][n // 4 * per:(n // 4 + 1) * per, :]
        for f in range(per):
            for c, cols in enumerate(blocks):
                xf_ref[c, (n * per + f) * lane_in:(n * per + f) * lane_in + patches, :] = ref[f, :, cols].astype(F32)
    group = 4
    for g in range(0, patches, group):
        for p in range(g, g + group):
            for c, cols in enumerate(blocks):
                h = xf_ref[c, pl.ds(p, steps, stride=lane_in), :]
                h_ref[p * steps:(p + 1) * steps, cols] = h.astype(BF16)
                att_ref[p * steps:(p + 1) * steps, cols] = (h + pos_ref[:, cols]).astype(BF16)
        rows = slice(g * steps, (g + group) * steps)
        qkv_ref[rows, :] = dot(att_ref[rows, :], wqkv_ref[...], NT).astype(BF16)
    low = pair_masks(steps)
    gap = jnp.zeros((pad, LANES), BF16)
    live = lax.broadcasted_iota(jnp.int32, (steps, LANES), 1) < steps

    def rows_of(p):
        return slice(p * steps, (p + 1) * steps)

    def scores(p, slot):
        rows = rows_of(p)
        for q in range(pairs):
            c0 = q * LANES
            k0, k1 = split_pair(qkv_ref[rows, width + c0:width + c0 + LANES], low)
            s_ref[slot, q] = dot(qkv_ref[rows, c0:c0 + LANES], jnp.concatenate([k0, gap, k1, gap], axis=0), NT)

    def softmax(slot):
        for q in range(pairs):
            inv = []
            for h in range(2):
                cols = slice(h * LANES, (h + 1) * LANES)
                sh = jnp.where(live, s_ref[slot, q, :, cols], NEG)
                e = jnp.exp2((sh - jnp.max(sh, axis=-1, keepdims=True)) * coef)
                inv.append(1.0 / jnp.sum(e, axis=-1, keepdims=True))
                p_ref[slot, q, :, cols] = e.astype(BF16)
            inv_ref[slot, q] = jnp.where(low, inv[0], inv[1])

    def values(p, slot):
        rows = rows_of(p)
        for q in range(pairs):
            c0 = q * LANES
            v0, v1 = split_pair(qkv_ref[rows, 2 * width + c0:2 * width + c0 + LANES], low)
            o = dot(p_ref[slot, q], jnp.concatenate([v0, gap, v1, gap], axis=0))
            att_ref[rows, c0:c0 + LANES] = (o * inv_ref[slot, q]).astype(BF16)

    scores(0, 0)
    scores(1, 1)
    softmax(0)

    for p in range(patches - 2):
        values(p, p % 2)
        softmax((p + 1) % 2)
        scores(p + 2, p % 2)
    values(patches - 2, 0)
    softmax(1)
    values(patches - 1, 1)
    wide = 2 * LANES
    for g in range(0, patches, group):
        rows = slice(g * steps, (g + group) * steps)
        for d in range(0, width, wide):
            branch = dot(att_ref[rows, :], wout_ref[:, d:d + wide])
            h2 = h_ref[rows, d:d + wide].astype(F32) + mod_ref[0, 2:3, d:d + wide] * branch
            for k in range(group):
                dst = slice((g + k) * lane_out, (g + k) * lane_out + steps)
                xf_ref[d // LANES, dst, :] = h2[k * steps:(k + 1) * steps, :LANES]
                xf_ref[d // LANES + 1, dst, :] = h2[k * steps:(k + 1) * steps, LANES:]
    span = pieces * per // splits
    for n in range(4 * pieces):
        for f in range(per):
            at = n // 4 * per + f
            ref = outs[at // span * 4 + n % 4]
            for c, cols in enumerate(blocks):
                ref[at % span, :, cols] = xf_ref[c, pl.ds(n * per + f, patches, stride=lane_out), :].astype(BF16)


def temporal_call(me, pieces, pos, modulation, wqkv, wout, video, splits, head_dim, patches=16):
    per, part, width = pieces[0].shape
    count = len(pieces) // 4
    steps = len(pieces) * per
    rows = steps * patches
    span = count * per // splits
    total = steps * part
    flops = 2 * total * (4 * width * width + 4 * LANES * width)
    pos_spec = lambda r: pl.BlockSpec((count * per, width), lambda i, me: (me[0] ^ r, 0))
    grid_spec = pltpu.PrefetchScalarGridSpec(
        num_scalar_prefetch=1,
        grid=(part // patches,),
        in_specs=[pl.BlockSpec((per, patches, width), lambda i, me: (0, i, 0))] * len(pieces)
        + [pos_spec(r) for r in range(4)]
        + [
            pl.BlockSpec((1, 6, width), lambda i, me: (video, 0, 0)),
            pl.BlockSpec(wqkv.shape, lambda i, me: (0, 0)),
            pl.BlockSpec(wout.shape, lambda i, me: (0, 0)),
        ],
        out_specs=[pl.BlockSpec((span, patches, width), lambda i, me: (0, i, 0))] * (4 * splits),
        scratch_shapes=[
            pltpu.VMEM((width // LANES, rows + LANES, LANES), F32),
            pltpu.VMEM((rows, width), BF16),
            pltpu.VMEM((rows, 3 * width), BF16),
            pltpu.VMEM((rows, width), BF16),
            pltpu.VMEM((2, width // LANES, steps, 2 * LANES), F32),
            pltpu.VMEM((2, width // LANES, steps, 2 * LANES), BF16),
            pltpu.VMEM((2, width // LANES, steps, LANES), F32),
            pltpu.VMEM((steps, width), F32),
        ],
    )
    return pl.pallas_call(
        functools.partial(temporal_kernel, head_dim, count, patches, splits),
        grid_spec=grid_spec,
        out_shape=[jax.ShapeDtypeStruct((span, part, width), BF16)] * (4 * splits),
        compiler_params=pltpu.CompilerParams(vmem_limit_bytes=VMEM_LIMIT),
        cost_estimate=pl.CostEstimate(flops=flops, bytes_accessed=4 * total * width, transcendentals=0),
        name=f"temporal_{video}",
    )(me, *pieces, *([pos] * 4), modulation, wqkv, wout)


def cross_kernel(head_dim, frames, text_len, steps, me_ref, *refs):
    ins = refs[:4]
    mod_ref, kk_ref, vv_ref, wq_ref, wo_ref, win_hbm, wmid_hbm = refs[4:11]
    out_ref, h_ref, q_ref, s_ref, p_ref, inv_ref, att_ref, new_ref, h3_ref, n_ref, g_ref, win_ref, wmid_ref, sems = refs[-14:]
    part, width = ins[0].shape[1:]
    tokens = 4 * part
    rows = frames * tokens
    hidden = win_ref.shape[1]
    pairs = width // LANES
    span = hidden // pairs
    wide = 2 * LANES
    coef = math.log2(math.e) * head_dim ** -0.5
    low = pair_masks(rows)
    live = lax.broadcasted_iota(jnp.int32, (rows, LANES), 1) < text_len

    def enter():
        for f in range(frames):
            for r in range(4):
                h_ref[f * tokens + r * part:f * tokens + (r + 1) * part, :] = ins[r][f]
        q_ref[...] = dot(h_ref[...], wq_ref[...], NT).astype(BF16)

    def scores(p):
        s_ref[p % 2] = dot(q_ref[:, p * LANES:(p + 1) * LANES], kk_ref[0, p], NT)

    def softmax(p):
        inv = []
        for h in range(2):
            cols = slice(h * LANES, (h + 1) * LANES)
            sh = jnp.where(live, s_ref[p % 2, :, cols], NEG)
            e = jnp.exp2((sh - jnp.max(sh, axis=-1, keepdims=True)) * coef)
            inv.append(1.0 / jnp.sum(e, axis=-1, keepdims=True))
            p_ref[p % 2, :, cols] = e.astype(BF16)
        inv_ref[p % 2] = jnp.where(low, inv[0], inv[1])

    def values(p):
        o = dot(p_ref[p % 2], vv_ref[0, p])
        att_ref[:, p * LANES:(p + 1) * LANES] = (o * inv_ref[p % 2]).astype(BF16)

    def expand(p):
        cols = slice(p * span, (p + 1) * span)
        a = dot(n_ref[...], win_ref[:, cols])
        t = jnp.tanh(a * (GELU_C + (GELU_C * 0.044715) * (a * a)))
        half = 0.5 * a
        g_ref[:, cols] = (half + half * t).astype(BF16)

    def attend_out():
        for d in range(0, width, wide):
            cols = slice(d, d + wide)
            new_ref[:, cols] = (h_ref[:, cols].astype(F32) + dot(att_ref[...], wo_ref[:, cols])).astype(BF16)

    def norm():
        n_ref[...] = (normalize(new_ref[...].astype(F32)) * (1.0 + mod_ref[0, 4:5, :]) + mod_ref[0, 3:4, :]).astype(BF16)

    def contract():
        for d in range(0, width, wide):
            cols = slice(d, d + wide)
            y = (h3_ref[:, cols].astype(F32) + mod_ref[0, 5:6, cols] * dot(g_ref[...], wmid_ref[:, cols])).astype(BF16)
            for f in range(frames):
                for r in range(4):
                    start = pl.multiple_of((me_ref[0] ^ r) * part, part)
                    out_ref[0, f, pl.ds(start, part), cols] = y[f * tokens + r * part:f * tokens + (r + 1) * part]

    def step(first, last):
        if not last:
            enter()
            scores(0)
        for p in range(pairs):
            if not last and p + 1 < pairs:
                scores(p + 1)
            if not first:
                expand(p)
            if not last:
                softmax(p)
                values(p)
        if not last:
            attend_out()
            norm()
        if not first:
            contract()
        if not last:
            h3_ref[...] = new_ref[...]

    loads = [pltpu.make_async_copy(win_hbm, win_ref, sems.at[0]), pltpu.make_async_copy(wmid_hbm, wmid_ref, sems.at[1])]
    i = pl.program_id(0)

    @pl.when(i == 0)
    def _():
        for load in loads:
            load.start()
        step(True, False)
        for load in loads:
            load.wait()

    pl.when(jnp.logical_and(i > 0, i < steps))(lambda: step(False, False))
    pl.when(i == steps)(lambda: step(False, True))


def cross_call(me, pieces, modulation, kk, vv, wq, wo, win, wmid, prev, out_shape, video, first, text_len, head_dim, frames=2):
    per, part, width = pieces[0].shape
    rows = frames * 4 * part
    hidden = win.shape[1]
    steps = per // frames
    base = first // frames
    whole = lambda a: pl.BlockSpec(a.shape, lambda i, me: (0, 0))
    in_specs = [pl.BlockSpec((frames, part, width), lambda i, me: (jnp.minimum(i, steps - 1), 0, 0))] * 4 + [
        pl.BlockSpec((1, 6, width), lambda i, me: (video, 0, 0)),
        pl.BlockSpec((1,) + kk.shape[1:], lambda i, me: (video, 0, 0, 0)),
        pl.BlockSpec((1,) + vv.shape[1:], lambda i, me: (video, 0, 0, 0)),
        whole(wq), whole(wo), pl.BlockSpec(memory_space=pl.ANY), pl.BlockSpec(memory_space=pl.ANY),
    ]
    args = [me, *pieces, modulation, kk, vv, wq, wo, win, wmid]
    aliases = {}
    if prev is not None:
        in_specs.append(pl.BlockSpec(memory_space=pl.ANY))
        aliases = {len(args): 0}
        args.append(prev)
    grid_spec = pltpu.PrefetchScalarGridSpec(
        num_scalar_prefetch=1,
        grid=(steps + 1,),
        in_specs=in_specs,
        out_specs=pl.BlockSpec((1, frames, 4 * part, width), lambda i, me: (video, base + jnp.maximum(i - 1, 0), 0, 0)),
        scratch_shapes=[
            pltpu.VMEM((rows, width), BF16),
            pltpu.VMEM((rows, width), BF16),
            pltpu.VMEM((2, rows, 2 * LANES), F32),
            pltpu.VMEM((2, rows, 2 * LANES), BF16),
            pltpu.VMEM((2, rows, LANES), F32),
            pltpu.VMEM((rows, width), BF16),
            pltpu.VMEM((rows, width), BF16),
            pltpu.VMEM((rows, width), BF16),
            pltpu.VMEM((rows, width), BF16),
            pltpu.VMEM((rows, hidden), BF16),
            pltpu.VMEM(win.shape, BF16),
            pltpu.VMEM(wmid.shape, BF16),
            pltpu.SemaphoreType.DMA((2,)),
        ],
    )
    total = per * 4 * part
    flops = 2 * total * (2 * width * width + 4 * LANES * width + 2 * width * hidden)
    return pl.pallas_call(
        functools.partial(cross_kernel, head_dim, frames, text_len, steps),
        grid_spec=grid_spec,
        out_shape=jax.ShapeDtypeStruct(out_shape, BF16),
        input_output_aliases=aliases,
        compiler_params=pltpu.CompilerParams(vmem_limit_bytes=VMEM_LIMIT),
        cost_estimate=pl.CostEstimate(flops=flops, bytes_accessed=4 * total * width, transcendentals=0),
        name=f"cross_{video}_{first}",
    )(*args)


def text_kernel(ctx_ref, wkv_ref, kk_ref, vv_ref):
    length, width = ctx_ref.shape[1:]
    kv = dot(ctx_ref[0], wkv_ref[...], NT)
    kv = jnp.concatenate([kv, jnp.zeros((LANES - length, 2 * width), F32)], axis=0).astype(BF16)
    low = pair_masks(LANES)
    for p in range(width // LANES):
        for ref, c0 in ((kk_ref, p * LANES), (vv_ref, width + p * LANES)):
            for h, half in enumerate(split_pair(kv[:, c0:c0 + LANES], low)):
                ref[0, p, h * LANES:(h + 1) * LANES, :] = half


def text_blocks(text_ctx, w_kv):
    videos, length, width = text_ctx.shape
    block = (1, width // LANES, 2 * LANES, LANES)
    return pl.pallas_call(
        text_kernel,
        grid=(videos,),
        in_specs=[pl.BlockSpec((1, length, width), lambda b: (b, 0, 0)), pl.BlockSpec(w_kv.shape, lambda b: (0, 0))],
        out_specs=[pl.BlockSpec(block, lambda b: (b, 0, 0, 0))] * 2,
        out_shape=[jax.ShapeDtypeStruct((videos,) + block[1:], BF16)] * 2,
        compiler_params=pltpu.CompilerParams(vmem_limit_bytes=VMEM_LIMIT),
        cost_estimate=pl.CostEstimate(flops=4 * videos * LANES * width * width, bytes_accessed=w_kv.size * 2, transcendentals=0),
        name="text",
    )(text_ctx, w_kv)


def solution(mesh):
    act_spec = P('dp', 'sp', None, None)
    row_spec = P('dp', None, None)
    rep_two = P(None, None)
    rep_three = P(None, None, None)
    rep_four = P(None, None, None, None)
    in_specs = (act_spec, row_spec, row_spec, rep_two, rep_four, rep_three, rep_four, rep_three, rep_three, rep_four, rep_three, rep_two, rep_two)
    def exchange(parts):
        return [parts[0]] + [lax.ppermute(parts[r], 'sp', [(i, i ^ r) for i in range(4)]) for r in range(1, 4)]

    def local_block(latents, text_ctx, modulation, pos_temporal, w_qkv_spatial, w_out_spatial, w_qkv_temporal, w_out_temporal, w_query_cross, w_kv_cross, w_out_cross, w_mlp_in, w_mlp_out):
        videos, frames, tokens, width = latents.shape
        head_dim = w_out_spatial.shape[1]
        index = lax.axis_index('sp')
        me = index.astype(jnp.int32)[None]
        flat_in = lambda w: w.reshape(-1, width)
        flat_out = lambda w: w.reshape(width, width)
        wqkv_s, wqkv_t, wq_c = flat_in(w_qkv_spatial), flat_in(w_qkv_temporal), flat_in(w_query_cross)
        wo_s, wo_t, wo_c = flat_out(w_out_spatial), flat_out(w_out_temporal), flat_out(w_out_cross)
        kk, vv = text_blocks(text_ctx, w_kv_cross.reshape(-1, width))
        gathered = []
        for b in range(videos):
            pieces = []
            for first, count in SPATIAL_CHUNKS[b]:
                parts = spatial_call(me, latents, modulation, wqkv_s, wo_s, b, first, count, head_dim)
                me, parts = lax.optimization_barrier((me, parts))
                pieces += exchange(parts)
            gathered.append(pieces)
        waiting, returned = [], {}

        def send_next(me):
            if waiting:
                key, parts = waiting.pop(0)
                me, parts = lax.optimization_barrier((me, parts))
                returned[key] = exchange(parts)
            return me

        for b in range(videos):
            parts = temporal_call(me, gathered[b], pos_temporal, modulation, wqkv_t, wo_t, b, SPLITS[b], head_dim)
            me, parts = lax.optimization_barrier((me, parts))
            waiting += [((b, n), parts[4 * n:4 * n + 4]) for n in range(SPLITS[b])]
            me = send_next(me)
        y = None
        for b in range(videos):
            for n in range(SPLITS[b]):
                y = cross_call(me, returned[b, n], modulation, kk, vv, wq_c, wo_c, w_mlp_in, w_mlp_out, y, latents.shape, b, n * frames // SPLITS[b], text_ctx.shape[1], head_dim)
                if waiting:
                    me, y = lax.optimization_barrier((me, y))
                    me = send_next(me)
        return y

    return jax.shard_map(local_block, mesh=mesh, in_specs=in_specs, out_specs=act_spec, check_vma=False)
```
